32 devices in a mesh: groups: 2 (over y), rows: 4 (over z), cols: 2 (over x), sub: 2 (over core).
Axes of the slice: x: 2, y: 2, z: 4, core: 2. Of those that a mesh axis runs over, the one named last changes fastest.
Arguments:
- stored_vectors: bfloat16 [3072, 8192], P(('cols', 'sub'), ('groups', 'rows')), parts along dimension 1, may hold values from -0.59765625 to 0.59765625
- previous_columns: bfloat16 [8192, 256], P(('groups', 'rows', 'cols', 'sub')), parts along dimension 0, may hold values from -3 to 3
- pivots: int32 [512], P('groups'), parts along dimension 0, may hold values from 0 to 4095, as said below
- diagonal: float32 [8192], P(('groups', 'rows', 'cols', 'sub')), parts along dimension 0, may hold values from 2 to 32
- ket_blocks: bfloat16 [128, 128, 256], P(('groups', 'rows', 'cols', 'sub')), parts along dimension 0, may hold values from -6 to 6
- shell_tags: int32 [128, 128], P(('groups', 'rows', 'cols', 'sub')), parts along dimension 0, may hold values from 0 to 3
- target_blocks: int32 [32, 4], P('groups'), parts along dimension 0, may hold values from 0 to 31, as said below
- block_counts: int32 [32], P('groups'), parts along dimension 0, may hold values from 0 to 4, as said below
- shell_norms: float32 [4], replicated, may hold values from 0.5 to 2
Outputs:
- new_vectors: bfloat16 [8192, 256], P(('groups', 'rows', 'cols', 'sub')), parts along dimension 0
- diag_out: float32 [8192], P(('groups', 'rows', 'cols', 'sub')), parts along dimension 0
- next_columns: bfloat16 [8192, 256], P(('groups', 'rows', 'cols', 'sub')), parts along dimension 0
The draws below stay inside these ranges and needn't reach their ends.
There are 2 independent parts, one for each index of `groups`. The reference program is written for one: setup_inputs(seed, part) draws one part's arguments, and reference() takes and returns one part's arrays. A program takes and returns all parts, laid end to end along the dimension named above; an argument that names none is the same for every part. Nothing has to cross between parts.
Inputs may be any that keep to these rules, and one draw needn't show every extreme that they name: `pivots`: 256 distinct AO pairs. `target_blocks`: the used slots of all owners name every block of the 32 blocks exactly once; a used slot's block lies on a device with the owner's cols and sub indices (blocks g * 2 to g * 2 + 1 lie on the device of linear index g, rows slowest; owner o is the device of linear index o). At most 1 of one owner's used slots go to one device, and some owner reaches that in every draw. Entries of unused slots are arbitrary blocks. `block_counts`: some owner uses all 4 slots in every draw.
All inputs are finite; a program needn't handle non-finite values.
Results may differ from the reference program's by a relative error of at most 0.0004.
Values may be sent and summed in bfloat16 or wider, within the bound.
A program may use at most 64 MiB of HBM per device.

```python
import math
import jax
import jax.numpy as jnp
from jax import lax

K = 3072
B = 256
BLK = 128
BLOCKS_DEV = 2
SHELL_TYPES = 4
CAP = 4
OWNERS = 16
PAIRS = 4096
N_ROWS = 4
N_COLS = 2
N_SUB = 2


def layout_draw(key):
    band_count = N_ROWS
    column = N_COLS * N_SUB
    per_device = BLOCKS_DEV
    slot_count = 2 * BLOCKS_DEV
    base = jax.random.fold_in(key, 11)
    keys = jax.random.split(base, 4)
    ranks = jnp.arange(band_count, dtype=jnp.int32)
    rank_counts = jnp.where(ranks == 0, slot_count, jnp.where(ranks == 1, 0, per_device)).astype(jnp.int32)
    rank_starts = (jnp.cumsum(rank_counts) - rank_counts).astype(jnp.int32)
    order = jax.vmap(lambda sub_key: jax.random.permutation(sub_key, band_count))(jax.random.split(keys[0], column)).astype(jnp.int32)
    lines = jnp.arange(column, dtype=jnp.int32)[:, None]
    counts = jnp.zeros((column, band_count), jnp.int32).at[lines, order].set(jnp.broadcast_to(rank_counts, (column, band_count)))
    starts = jnp.zeros((column, band_count), jnp.int32).at[lines, order].set(jnp.broadcast_to(rank_starts, (column, band_count)))
    total = band_count * per_device
    receiver_order = jax.vmap(lambda sub_key: jax.random.permutation(sub_key, band_count))(jax.random.split(keys[1], column)).astype(jnp.int32)
    within_order = jax.vmap(lambda sub_key: jax.random.permutation(sub_key, per_device))(jax.random.split(keys[2], column)).astype(jnp.int32)
    slots = jnp.arange(slot_count, dtype=jnp.int32)
    position = jnp.minimum(starts[:, :, None] + slots[None, None, :], total - 1)
    receiver_spread = jnp.broadcast_to(receiver_order[:, None, :], (column, band_count, band_count))
    receiver = jnp.take_along_axis(receiver_spread, position % band_count, axis=2)
    within_spread = jnp.broadcast_to(within_order[:, None, :], (column, band_count, per_device))
    within = jnp.take_along_axis(within_spread, position // band_count, axis=2)
    target = (receiver * column + jnp.arange(column, dtype=jnp.int32)[:, None, None]) * per_device + within
    filler = jax.random.randint(keys[3], (column, band_count, slot_count), 0, band_count * column * per_device).astype(jnp.int32)
    valid = slots[None, None, :] < counts[:, :, None]
    target = jnp.where(valid, target, filler)
    target = jnp.transpose(target, (1, 0, 2)).reshape(band_count * column, slot_count)
    owner_counts = jnp.transpose(counts, (1, 0)).reshape(band_count * column)
    return (target.astype(jnp.int32), owner_counts.astype(jnp.int32))


def draw_target_blocks(key, part):
    return layout_draw(key)[0]


def draw_block_counts(key, part):
    return layout_draw(key)[1]


def draw_pivots(key, part):
    chosen = jax.random.permutation(jax.random.fold_in(key, 5), PAIRS)
    return chosen[:B].astype(jnp.int32)


def place_ends(entries, key, smallest, largest):
    longest = entries.shape.index(max(entries.shape))
    spots = []
    for shift in (0, 1):
        where = [jax.random.randint(jax.random.fold_in(key, axis), (), 0, length) for axis, length in enumerate(entries.shape)]
        where[longest] = (where[longest] + shift) % entries.shape[longest]
        spots.append(tuple(where))
    return entries.at[spots[0]].set(smallest).at[spots[1]].set(largest)


def block_levels(rng, extent, cuts, low, high):
    gain = 1.0
    for dim, shards_of in cuts:
        draws = jax.random.uniform(jax.random.fold_in(jax.random.fold_in(rng, 6), dim), (shards_of,), jnp.float32, low / len(cuts), high / len(cuts))
        gain = gain * jnp.repeat(jnp.exp(draws), extent[dim] // shards_of).reshape((-1,) + (1,) * (len(extent) - 1 - dim))
    return gain


def centred(own_key, extent, scale, most, pieces=(), kind=jnp.bfloat16):
    entries = scale * jax.random.normal(own_key, extent, jnp.float32)
    if pieces:
        entries = entries * block_levels(own_key, extent, pieces, -0.22, 0.18)
    return jnp.clip(entries, -most, most).astype(kind)


def setup_inputs(seed: int = 0, part: int = 0) -> dict:
    seeds = jax.random.split(jax.random.key(seed), 10)
    part_keys = jax.random.split(jax.random.fold_in(seeds[9], part), 10)
    return {
        "stored_vectors": centred(part_keys[0], (K, PAIRS), 0.1, 0.59765625, ((0, 4), (1, 4))),
        "previous_columns": centred(part_keys[1], (PAIRS, B), 0.5, 3.0, ((0, 16),)),
        "pivots": draw_pivots(jax.random.fold_in(jax.random.fold_in(seeds[9], part), 71), part),
        "diagonal": jnp.clip(jnp.exp(math.log(32.0) - 2.7725887 * jax.random.uniform(part_keys[3], (PAIRS,), jnp.float32) ** block_levels(part_keys[3], (PAIRS,), ((0, 16),), -0.2, 0.2)), 2.0, 32.0),
        "ket_blocks": centred(part_keys[4], (OWNERS * CAP, BLK, B), 1.0, 6.0, ((0, 16),)),
        "shell_tags": place_ends(jax.random.randint(part_keys[5], (OWNERS * CAP, BLK), 0, SHELL_TYPES), jax.random.fold_in(part_keys[5], 1), 0, SHELL_TYPES - 1).astype(jnp.int32),
        "target_blocks": draw_target_blocks(jax.random.fold_in(jax.random.fold_in(seeds[9], part), 71), part),
        "block_counts": draw_block_counts(jax.random.fold_in(jax.random.fold_in(seeds[9], part), 71), part),
        "shell_norms": jnp.clip(jnp.exp(jax.random.uniform(seeds[8], (SHELL_TYPES,), jnp.float32, math.log(0.5), math.log(2.0))), 0.5, 2.0),
    }


def reference(stored_vectors, previous_columns, pivots, diagonal, ket_blocks, shell_tags, target_blocks, block_counts, shell_norms):
    kinds = jnp.arange(shell_norms.shape[0], dtype=jnp.int32)
    factor = lax.optimization_barrier(jnp.sum(jnp.where(shell_tags[..., None] == kinds, shell_norms, jnp.float32(0.0)), axis=-1))
    fresh = (ket_blocks.astype(jnp.float32) * factor[..., None]).astype(jnp.bfloat16)
    slots = jnp.arange(CAP, dtype=jnp.int32)
    valid = slots[None, :] < block_counts[:, None]
    blocks_total = PAIRS // BLK
    placing = jnp.where(valid, target_blocks, blocks_total).reshape(-1).astype(jnp.int32)
    placed = jnp.zeros((blocks_total, BLK, B), jnp.bfloat16).at[placing].set(fresh, mode='drop')
    next_columns = placed.reshape(PAIRS, B)
    pivot_rows = stored_vectors[:, pivots]
    groups_count = N_COLS * N_SUB
    width = K // groups_count
    product = jnp.zeros((PAIRS, B), jnp.float32)
    for group in range(groups_count):
        block_vectors = stored_vectors[group * width:(group + 1) * width]
        block_pivots = pivot_rows[group * width:(group + 1) * width]
        partial_sum = jnp.dot(block_vectors.T, block_pivots, preferred_element_type=jnp.float32)
        product = product + partial_sum
    residual_cols = previous_columns.astype(jnp.float32) - product
    pivot_diag = diagonal[pivots]
    scaled = residual_cols / jnp.sqrt(pivot_diag)[None, :]
    new_vectors = scaled.astype(jnp.bfloat16)
    diag_out = diagonal - lax.optimization_barrier(jnp.sum(scaled * scaled, axis=1))
    return (new_vectors, diag_out, next_columns)
```

```python
import functools

import jax
import jax.numpy as jnp
from jax import lax
from jax.experimental import pallas as pl
from jax.experimental.pallas import tpu as pltpu
from jax.sharding import PartitionSpec as P

MESH = pl.DeviceIdType.MESH
LANES = 128
PART = 256
KET_LOW, KET_HIGH = 0, 8
REDUCE_LAG = (2, 4)
HEAD = 2
DEFER = 4
GROUPS = (2,) * 8
PD_SUB, PD_COLS = 4, 8


def column_of(row):
    return jnp.transpose(jnp.broadcast_to(row, (LANES, row.shape[1])))


def kernel(
    sizes,
    vec_hbm, prev_hbm, piv_hbm, diag_hbm, ket_hbm, tags_hbm, targets_hbm, counts_hbm, norms_hbm,
    new_ref, diag_out_ref, next_ref,
    piv_ref, diag_ref, tags_ref, targets_ref, counts_ref, norms_ref,
    vec, prev, ket, hot, own, fwd_r, fwd_l, from_l, from_r,
    pivot_t, prev_t, sub_out, sub_in, mine, col_out, col_in, scaled_t,
    stage, landed, pd_z, pd_s, pd_c, pd_own_s, pd_own_c,
    load_sem, vec_sem, zr_send, zl_send, l_recv, r_recv, sub_send, sub_recv, col_send, col_recv,
    ket_send, ket_recv, pdz_send, pdz_recv, pds_send, pds_recv, pdc_send, pdc_recv,
):
    n_rows, n_cols, n_sub, hop_lead, hop_bias, groups = sizes
    z, x, s = lax.axis_index("rows"), lax.axis_index("cols"), lax.axis_index("sub")
    column_size = n_cols * n_sub
    column = x * n_sub + s
    device = z * column_size + column
    slot_count, block_rows, batch = ket_hbm.shape
    rows_here = prev_hbm.shape[0]
    per_device = rows_here // block_rows
    width, band_rows = vec_hbm.shape
    z_chunks, z_rows = own.shape[0], own.shape[1]
    last = len(groups) - 1

    k_part = PART if width % PART == 0 else width
    load_piv = pltpu.make_async_copy(piv_hbm, piv_ref, load_sem.at[0])
    load_piv.start()
    load_diag = pltpu.make_async_copy(diag_hbm, diag_ref, load_sem.at[1])
    load_diag.start()
    load_vec = []
    for p in range(width // k_part):
        at = pl.ds(p * k_part, k_part)
        load_vec.append(pltpu.make_async_copy(vec_hbm.at[at], vec.at[at], vec_sem.at[p]))
        load_vec[-1].start()
    load_ket = pltpu.make_async_copy(ket_hbm, ket, load_sem.at[2])
    load_tags = pltpu.make_async_copy(tags_hbm, tags_ref, load_sem.at[3])
    load_targets = pltpu.make_async_copy(targets_hbm, targets_ref, load_sem.at[4])
    load_counts = pltpu.make_async_copy(counts_hbm, counts_ref, load_sem.at[5])
    load_norms = pltpu.make_async_copy(norms_hbm, norms_ref, load_sem.at[6])
    load_prev = pltpu.make_async_copy(prev_hbm, prev, load_sem.at[7])
    for c in (load_tags, load_norms, load_targets, load_counts, load_ket, load_prev):
        c.start()

    barrier = pltpu.get_barrier_semaphore()
    for name, here, count in (("rows", z, n_rows), ("cols", x, n_cols), ("sub", s, n_sub)):
        for d in range(1, count):
            pl.semaphore_signal(
                barrier, inc=1, device_id={name: lax.rem(here + d, count)}, device_id_type=MESH
            )

    load_piv.wait()
    piv_col = column_of(piv_ref[...].astype(jnp.float32)).astype(jnp.int32) - z * band_rows
    lane = lax.broadcasted_iota(jnp.int32, (batch, LANES), 1)
    for t in range(band_rows // LANES):
        hot[:, t * LANES:(t + 1) * LANES] = (piv_col == lane + t * LANES).astype(
            jnp.float32).astype(jnp.bfloat16)

    def ket_copy(d):
        return pltpu.make_async_remote_copy(
            src_ref=stage.at[d], dst_ref=landed.at[z], send_sem=ket_send.at[d],
            recv_sem=ket_recv.at[z], device_id={"rows": lax.rem(z + d, n_rows)},
            device_id_type=MESH)

    inner = (z > 0) & (z < n_rows - 1)

    def z_copy(src, dst, send, recv, q, dz):
        return pltpu.make_async_remote_copy(
            src_ref=src.at[q], dst_ref=dst.at[q], send_sem=send.at[q], recv_sem=recv.at[q],
            device_id={"rows": lax.rem(z + dz + n_rows, n_rows)}, device_id_type=MESH)

    def arrived(dst, sem):
        pltpu.make_async_remote_copy(
            src_ref=dst, dst_ref=dst, send_sem=sem, recv_sem=sem,
            device_id={"sub": lax.rem(s + 1, n_sub)}, device_id_type=MESH).wait_recv()

    load_diag.wait()
    diag_col = column_of(diag_ref[...])
    row = lax.broadcasted_iota(jnp.int32, (rows_here, LANES), 0) + device * rows_here
    for h in range(batch // LANES):
        cut = slice(h * LANES, (h + 1) * LANES)
        share = jnp.sum(jnp.where(piv_ref[:, cut] == row, diag_col, 0.0), axis=0, keepdims=True)
        pd_z[n_rows, :, cut] = share

    def pd_copies(src, dst, send, recv, name, here, count):
        return [pltpu.make_async_remote_copy(
            src_ref=src, dst_ref=dst.at[here], send_sem=send.at[d], recv_sem=recv.at[here],
            device_id={name: lax.rem(here + d, count)}, device_id_type=MESH)
            for d in range(1, count)]

    pdz = pd_copies(pd_z.at[n_rows], pd_z, pdz_send, pdz_recv, "rows", z, n_rows)
    pds = pd_copies(pd_own_s, pd_s, pds_send, pds_recv, "sub", s, n_sub)
    pdc = pd_copies(pd_own_c, pd_c, pdc_send, pdc_recv, "cols", x, n_cols)

    def gather(first, count):
        rows = slice(first * z_rows, (first + count) * z_rows)
        for p in range(width // k_part):
            if first == 0:
                load_vec[p].wait()
            at = slice(p * k_part, (p + 1) * k_part)
            got = lax.dot_general(
                hot[rows, :], vec[at, :], (((1,), (1,)), ((), ())),
                preferred_element_type=jnp.float32).astype(jnp.bfloat16)
            own[first:first + count, :, at] = got.reshape(count, z_rows, k_part)

    def send_own(first, count):
        @pl.when(z == n_rows - 1)
        def _():
            for q in range(first, first + count):
                z_copy(own, from_r, zl_send, r_recv, q, -1).start()

        @pl.when(z == 0)
        def _():
            for q in range(first, first + count):
                z_copy(own, from_l, zr_send, l_recv, q, 1).start()

    head = HEAD
    gather(0, head)
    pl.semaphore_wait(barrier, n_rows + n_cols + n_sub - 3)
    send_own(0, head)
    for c in pdz:
        c.start()
    gather(head, z_chunks - head)
    send_own(head, z_chunks - head)

    @pl.when(z == 0)
    def _():
        fwd_r[...] = own[...]

    load_tags.wait()
    load_norms.wait()
    tags = tags_ref[...]
    factor = jnp.zeros(tags.shape, jnp.float32)
    for kind in range(norms_ref.shape[0]):
        factor = jnp.where(tags == kind, norms_ref[kind], factor)
    load_ket.wait()
    for slot in range(slot_count):
        scale = column_of(factor[slot:slot + 1, :])
        for h in range(batch // LANES):
            part = (slot, slice(None), slice(h * LANES, (h + 1) * LANES))
            ket[part] = (ket[part].astype(jnp.float32) * scale).astype(jnp.bfloat16)
    load_targets.wait()
    load_counts.wait()
    used = counts_ref[device]

    def stage_for(band):
        low = (band * column_size + column) * per_device
        chosen = jnp.int32(0)
        for slot in range(slot_count):
            target = targets_ref[slot, device]
            fits = (slot < used) & (target >= low) & (target < low + per_device)
            chosen = jnp.where(fits, jnp.int32(slot), chosen)
        return ket[chosen]

    landed[z] = stage_for(z)
    for d in range(1, n_rows):
        stage[d] = stage_for(lax.rem(z + d, n_rows))

    @pl.when(inner)
    def _():
        for d in range(1, n_rows):
            ket_copy(d).start()

    def pd_total(first, dst, recv, here, count):
        total = first[...]
        for d in range(1, count):
            other = lax.rem(here + d, count)
            arrived(dst.at[other], recv.at[other])
            total = total + dst[other]
        return total

    load_prev.wait()
    prev_t[...] = jnp.transpose(prev[...].astype(jnp.float32))

    tilt = jnp.where(inner, hop_lead * (2 * z - (n_rows - 1)) + hop_bias, 0)
    wait_l = jnp.clip(tilt, 0, z_chunks)
    wait_r = jnp.clip(-tilt, 0, z_chunks)
    lag = jnp.maximum(wait_l, wait_r)
    defer = jnp.where(inner, DEFER, 0)
    reduce_lag = jnp.where(s == 0, REDUCE_LAG[0], REDUCE_LAG[1])
    def chip_rows(g):
        first, count = groups[g]
        return pl.ds(first * z_rows * n_cols, count * z_rows * n_cols)

    def group_rows(g):
        first, count = groups[g]
        return pl.ds(first * z_rows, count * z_rows)

    def sub_copy(g, d):
        return pltpu.make_async_remote_copy(
            src_ref=sub_out.at[d, chip_rows(g)], dst_ref=sub_in.at[s, chip_rows(g)],
            send_sem=sub_send.at[g, d], recv_sem=sub_recv.at[g, s],
            device_id={"sub": lax.rem(s + d, n_sub)}, device_id_type=MESH)

    def col_copy(g, d):
        return pltpu.make_async_remote_copy(
            src_ref=col_out.at[d, group_rows(g)], dst_ref=col_in.at[x, group_rows(g)],
            send_sem=col_send.at[g, d], recv_sem=col_recv.at[g, x],
            device_id={"cols": lax.rem(x + d, n_cols)}, device_id_type=MESH)

    def block_dot(pivot_rows_t, col, sub):
        at = pl.multiple_of((col * n_sub + sub) * rows_here, LANES)
        return jnp.dot(
            pivot_rows_t, vec[:, pl.ds(at, rows_here)], preferred_element_type=jnp.float32)

    def chip_part(g, c):
        first, count = groups[g]
        return pl.ds((first * n_cols + c * count) * z_rows, count * z_rows)

    def multiply(g):
        first, count = groups[g]
        chunks = slice(first, first + count)

        @pl.when(z < n_rows - 1)
        def _():
            pivot_t[chunks] = fwd_r[chunks] + from_r[chunks]

        @pl.when(z == n_rows - 1)
        def _():
            pivot_t[chunks] = fwd_r[chunks]

        pt = pivot_t[chunks].reshape(count * z_rows, width)
        for d in range(1, n_sub):
            for c in range(n_cols):
                sub_out[d, chip_part(g, c)] = block_dot(
                    pt, lax.rem(x + c, n_cols), lax.rem(s + d, n_sub))
            sub_copy(g, d).start()
        for c in range(1, n_cols):
            col_out[c, group_rows(g)] = block_dot(pt, lax.rem(x + c, n_cols), s)
        mine[group_rows(g)] = block_dot(pt, x, s)

    def reduce_chip(g):
        for d in range(1, n_sub):
            other = lax.rem(s + d, n_sub)
            arrived(sub_in.at[other, chip_rows(g)], sub_recv.at[g, other])
        for c in range(1, n_cols):
            total = col_out[c, group_rows(g)]
            for d in range(1, n_sub):
                total = total + sub_in[lax.rem(s + d, n_sub), chip_part(g, c)]
            col_out[c, group_rows(g)] = total
            col_copy(g, c).start()
        total = mine[group_rows(g)]
        for d in range(1, n_sub):
            total = total + sub_in[lax.rem(s + d, n_sub), chip_part(g, 0)]
        mine[group_rows(g)] = total

    def step(t, carry):
        q_l, q_r, q_m = t - wait_l, t - wait_r, t - lag - defer

        @pl.when((z > 0) & (q_l >= 0) & (q_l < z_chunks))
        def _():
            z_copy(fwd_r, from_l, zr_send, l_recv, q_l, 1).wait_recv()
            fwd_r[q_l] = from_l[q_l] + own[q_l]

            @pl.when(z < n_rows - 1)
            def _():
                z_copy(fwd_r, from_l, zr_send, l_recv, q_l, 1).start()

        @pl.when((z < n_rows - 1) & (q_r >= 0) & (q_r < z_chunks))
        def _():
            z_copy(fwd_l, from_r, zl_send, r_recv, q_r, -1).wait_recv()

            @pl.when(z > 0)
            def _():
                fwd_l[q_r] = from_r[q_r] + own[q_r]
                z_copy(fwd_l, from_r, zl_send, r_recv, q_r, -1).start()

        @pl.when((z == n_rows - 1) & (t == KET_HIGH))
        def _():
            for d in reversed(range(1, n_rows)):
                ket_copy(d).start()

        @pl.when((z == 0) & (t == KET_LOW))
        def _():
            for d in range(1, n_rows):
                ket_copy(d).start()

        for g in range(last + 1):
            @pl.when(q_m == sum(groups[g]) - 1)
            def _():
                multiply(g)

        for g in range(last + 1):
            @pl.when(q_m == jnp.minimum(sum(groups[g]) - 1 + reduce_lag, z_chunks - 1))
            def _():
                reduce_chip(g)

        @pl.when(t == PD_SUB)
        def _():
            pd_own_s[...] = pd_total(pd_z.at[n_rows], pd_z, pdz_recv, z, n_rows)
            for c in pds:
                c.start()

        @pl.when(t == PD_COLS)
        def _():
            pd_own_c[...] = pd_total(pd_own_s, pd_s, pds_recv, s, n_sub)
            for c in pdc:
                c.start()

        return carry

    lax.fori_loop(0, z_chunks + lag + defer, step, 0)

    pivot_diag = pd_total(pd_own_c, pd_c, pdc_recv, x, n_cols)
    inverse = 1.0 / jnp.sqrt(column_of(pivot_diag[0:1, :]))
    total_sq = jnp.zeros((1, rows_here), jnp.float32)
    written = 0
    for g in range(last + 1):
        if g == last:
            for d in range(1, n_rows):
                other = lax.rem(z + d, n_rows)
                arrived(landed.at[other], ket_recv.at[other])
            for place in range(per_device):
                block = device * per_device + place
                source = jnp.int32(0)
                for band in range(n_rows):
                    owner = band * column_size + column
                    for slot in range(slot_count):
                        fits = (slot < counts_ref[owner]) & (targets_ref[slot, owner] == block)
                        source = jnp.where(fits, jnp.int32(band), source)
                next_ref[place * block_rows:(place + 1) * block_rows, :] = landed[source]
        total = mine[group_rows(g)]
        for c in range(1, n_cols):
            other = lax.rem(x + c, n_cols)
            arrived(col_in.at[other, group_rows(g)], col_recv.at[g, other])
            total = total + col_in[other, group_rows(g)]
        first, count = groups[g]
        rows = slice(first * z_rows, (first + count) * z_rows)
        for h in range(rows_here // LANES):
            cut = slice(h * LANES, (h + 1) * LANES)
            scaled_t[rows, cut] = (prev_t[rows, cut] - total[:, cut]) * inverse[rows, :]
        scaled = scaled_t[rows, :]
        total_sq = total_sq + jnp.sum(scaled * scaled, axis=0, keepdims=True)
        ready = sum(groups[g]) * z_rows // LANES * LANES if g < last else batch
        if ready > written:
            done = slice(written, ready)
            new_ref[:, done] = jnp.transpose(scaled_t[done, :]).astype(jnp.bfloat16)
            written = ready
    diag_out_ref[...] = diag_ref[...] - total_sq

    for c in pdz + pds + pdc:
        c.wait_send()
    for d in range(1, n_rows):
        ket_copy(d).wait_send()

    @pl.when(z < n_rows - 1)
    def _():
        for q in range(z_chunks):
            z_copy(own, from_l, zr_send, l_recv, q, 1).wait_send()

    @pl.when(z > 0)
    def _():
        for q in range(z_chunks):
            z_copy(own, from_r, zl_send, r_recv, q, -1).wait_send()

    for g in range(last + 1):
        for d in range(1, n_sub):
            sub_copy(g, d).wait_send()
        for c in range(1, n_cols):
            col_copy(g, c).wait_send()


def flush(new_ref, diag_ref, next_ref, new_hbm, diag_hbm, next_hbm, sem):
    copies = [
        pltpu.make_async_copy(new_ref, new_hbm, sem.at[0]),
        pltpu.make_async_copy(next_ref, next_hbm, sem.at[1]),
        pltpu.make_async_copy(diag_ref, diag_hbm, sem.at[2]),
    ]
    for c in copies:
        c.start()
    for c in copies:
        c.wait()


def body(mesh_sizes, vectors, previous, pivots, diagonal, ket_blocks, tags, targets, counts, norms):
    n_rows, n_cols, n_sub = mesh_sizes
    width, band_rows = vectors.shape
    rows_here, batch = previous.shape
    slot_count, block_rows, _ = ket_blocks.shape
    z_chunks, hop_lead, hop_bias = 16, 6, 1
    z_rows, m_chunks = batch // z_chunks, len(GROUPS)
    groups = tuple((sum(GROUPS[:g]), GROUPS[g]) for g in range(m_chunks))
    f32, bf16, dma = jnp.float32, jnp.bfloat16, pltpu.SemaphoreType.DMA
    line = pltpu.VMEM((z_chunks, z_rows, width), bf16)
    small = pltpu.VMEM((1, batch), f32)
    scratch = [
        pltpu.VMEM((1, batch), jnp.int32), pltpu.VMEM((1, rows_here), f32),
        pltpu.VMEM(tags.shape, jnp.int32), pltpu.SMEM(targets.shape[::-1], jnp.int32),
        pltpu.SMEM(counts.shape, jnp.int32), pltpu.SMEM(norms.shape, f32),
        pltpu.VMEM(vectors.shape, bf16), pltpu.VMEM(previous.shape, bf16),
        pltpu.VMEM(ket_blocks.shape, bf16), pltpu.VMEM((batch, band_rows), bf16),
        line, line, line, line, line, line,
        pltpu.VMEM((batch, rows_here), f32),
        pltpu.VMEM((n_sub, n_cols * batch, rows_here), f32),
        pltpu.VMEM((n_sub, n_cols * batch, rows_here), f32),
        pltpu.VMEM((batch, rows_here), f32),
        pltpu.VMEM((n_cols, batch, rows_here), f32),
        pltpu.VMEM((n_cols, batch, rows_here), f32),
        pltpu.VMEM((batch, rows_here), f32),
        pltpu.VMEM((n_rows, block_rows, batch), bf16),
        pltpu.VMEM((n_rows, block_rows, batch), bf16),
        pltpu.VMEM((n_rows + 1, 1, batch), f32), pltpu.VMEM((n_sub, 1, batch), f32),
        pltpu.VMEM((n_cols, 1, batch), f32), small, small,
        dma((8,)), dma((max(width // PART, 1),)), dma((z_chunks,)), dma((z_chunks,)), dma((z_chunks,)), dma((z_chunks,)),
        dma((m_chunks, n_sub)), dma((m_chunks, n_sub)),
        dma((m_chunks, n_cols)), dma((m_chunks, n_cols)),
        dma((n_rows,)), dma((n_rows,)), dma((n_rows,)), dma((n_rows,)),
        dma((n_sub,)), dma((n_sub,)), dma((n_cols,)), dma((n_cols,)),
    ]
    hbm = pl.BlockSpec(memory_space=pl.ANY)
    vmem = pl.BlockSpec(memory_space=pltpu.VMEM)
    new_vectors, diag_out, next_columns = pl.pallas_call(
        functools.partial(kernel, (n_rows, n_cols, n_sub, hop_lead, hop_bias, groups)),
        out_shape=(
            pltpu.VMEM((rows_here, batch), bf16),
            pltpu.VMEM((1, rows_here), f32),
            pltpu.VMEM((rows_here, batch), bf16),
        ),
        in_specs=[hbm] * 9,
        out_specs=(vmem, vmem, vmem),
        scratch_shapes=scratch,
        compiler_params=pltpu.CompilerParams(
            collective_id=0, has_side_effects=True, vmem_limit_bytes=63 * 1024 * 1024),
    )(
        vectors, previous, pivots.reshape(1, batch), diagonal.reshape(1, rows_here),
        ket_blocks, tags, targets.T, counts, norms,
    )
    new_vectors, diag_out, next_columns = pl.pallas_call(
        flush,
        out_shape=(
            jax.ShapeDtypeStruct((rows_here, batch), bf16),
            jax.ShapeDtypeStruct((1, rows_here), f32),
            jax.ShapeDtypeStruct((rows_here, batch), bf16),
        ),
        in_specs=[vmem] * 3,
        out_specs=(hbm, hbm, hbm),
        scratch_shapes=[dma((3,))],
        compiler_params=pltpu.CompilerParams(vmem_limit_bytes=1024 * 1024),
    )(new_vectors, diag_out, next_columns)
    return new_vectors, diag_out.reshape(rows_here), next_columns


def solution(mesh):
    sizes = tuple(mesh.shape[name] for name in ("rows", "cols", "sub"))
    return jax.shard_map(
        functools.partial(body, sizes),
        mesh=mesh,
        in_specs=(
            P(("cols", "sub"), ("groups", "rows")),
            P(("groups", "rows", "cols", "sub"), None),
            P("groups"),
            P(("groups", "rows", "cols", "sub")),
            P(("groups", "rows", "cols", "sub"), None, None),
            P(("groups", "rows", "cols", "sub"), None),
            P("groups", None),
            P("groups"),
            P(),
        ),
        out_specs=(
            P(("groups", "rows", "cols", "sub"), None),
            P(("groups", "rows", "cols", "sub")),
            P(("groups", "rows", "cols", "sub"), None),
        ),
        check_vma=False,
    )
```

```python
import functools

import jax
import jax.numpy as jnp
from jax import lax
from jax.experimental import pallas as pl
from jax.experimental.pallas import tpu as pltpu
from jax.sharding import PartitionSpec as P

MESH = pl.DeviceIdType.MESH
LANES = 128
PART = 256
KET_LOW, KET_HIGH = (0, 2), (4, 3)
REDUCE_LAG = (1, 5)
HEAD = 2
DEFER = 4
PER = 2
PD_SUB, PD_COLS = 4, 8


def column_of(row):
    return jnp.transpose(jnp.broadcast_to(row, (LANES, row.shape[1])))


def kernel(
    sizes,
    vec_hbm, prev_hbm, piv_hbm, diag_hbm, ket_hbm, tags_hbm, targets_hbm, counts_hbm, norms_hbm,
    new_ref, diag_out_ref, next_ref,
    piv_ref, diag_ref, tags_ref, targets_ref, counts_ref, norms_ref,
    vec, prev, ket, hot, own, fwd_r, fwd_l, from_l, from_r,
    pivot_t, prev_t, sub_out, sub_in, mine, col_out, col_in, scaled_t, inverse,
    stage, landed, pd_z, pd_s, pd_c, pd_own_s, pd_own_c,
    load_sem, vec_sem, zr_send, zl_send, l_recv, r_recv, sub_send, sub_recv, col_send, col_recv,
    ket_send, ket_recv, pdz_send, pdz_recv, pds_send, pds_recv, pdc_send, pdc_recv,
):
    n_rows, n_cols, n_sub, hop_lead, hop_bias, per = sizes
    z, x, s = lax.axis_index("rows"), lax.axis_index("cols"), lax.axis_index("sub")
    column_size = n_cols * n_sub
    column = x * n_sub + s
    device = z * column_size + column
    slot_count, block_rows, batch = ket_hbm.shape
    rows_here = prev_hbm.shape[0]
    per_device = rows_here // block_rows
    width, band_rows = vec_hbm.shape
    z_chunks, z_rows = own.shape[0], own.shape[1]
    groups = z_chunks // per
    last = groups - 1
    g_rows = per * z_rows

    k_part = PART if width % PART == 0 else width
    load_piv = pltpu.make_async_copy(piv_hbm, piv_ref, load_sem.at[0])
    load_piv.start()
    load_diag = pltpu.make_async_copy(diag_hbm, diag_ref, load_sem.at[1])
    load_diag.start()
    load_vec = []
    for p in range(width // k_part):
        at = pl.ds(p * k_part, k_part)
        load_vec.append(pltpu.make_async_copy(vec_hbm.at[at], vec.at[at], vec_sem.at[p]))
        load_vec[-1].start()
    load_ket = pltpu.make_async_copy(ket_hbm, ket, load_sem.at[2])
    load_tags = pltpu.make_async_copy(tags_hbm, tags_ref, load_sem.at[3])
    load_targets = pltpu.make_async_copy(targets_hbm, targets_ref, load_sem.at[4])
    load_counts = pltpu.make_async_copy(counts_hbm, counts_ref, load_sem.at[5])
    load_norms = pltpu.make_async_copy(norms_hbm, norms_ref, load_sem.at[6])
    load_prev = pltpu.make_async_copy(prev_hbm, prev, load_sem.at[7])
    for c in (load_tags, load_norms, load_targets, load_counts, load_ket, load_prev):
        c.start()

    barrier = pltpu.get_barrier_semaphore()
    for name, here, count in (("rows", z, n_rows), ("cols", x, n_cols), ("sub", s, n_sub)):
        for d in range(1, count):
            pl.semaphore_signal(
                barrier, inc=1, device_id={name: lax.rem(here + d, count)}, device_id_type=MESH
            )

    load_piv.wait()
    piv_col = column_of(piv_ref[...].astype(jnp.float32)).astype(jnp.int32) - z * band_rows
    lane = lax.broadcasted_iota(jnp.int32, (batch, LANES), 1)
    for t in range(band_rows // LANES):
        hot[:, t * LANES:(t + 1) * LANES] = (piv_col == lane + t * LANES).astype(
            jnp.float32).astype(jnp.bfloat16)

    def ket_copy(d):
        return pltpu.make_async_remote_copy(
            src_ref=stage.at[d], dst_ref=landed.at[z], send_sem=ket_send.at[d],
            recv_sem=ket_recv.at[z], device_id={"rows": lax.rem(z + d, n_rows)},
            device_id_type=MESH)

    inner = (z > 0) & (z < n_rows - 1)

    def z_copy(src, dst, send, recv, q, dz):
        return pltpu.make_async_remote_copy(
            src_ref=src.at[q], dst_ref=dst.at[q], send_sem=send.at[q], recv_sem=recv.at[q],
            device_id={"rows": lax.rem(z + dz + n_rows, n_rows)}, device_id_type=MESH)

    def arrived(dst, sem):
        pltpu.make_async_remote_copy(
            src_ref=dst, dst_ref=dst, send_sem=sem, recv_sem=sem,
            device_id={"sub": lax.rem(s + 1, n_sub)}, device_id_type=MESH).wait_recv()

    load_diag.wait()
    diag_col = column_of(diag_ref[...])
    row = lax.broadcasted_iota(jnp.int32, (rows_here, LANES), 0) + device * rows_here
    for h in range(batch // LANES):
        cut = slice(h * LANES, (h + 1) * LANES)
        share = jnp.sum(jnp.where(piv_ref[:, cut] == row, diag_col, 0.0), axis=0, keepdims=True)
        pd_z[n_rows, :, cut] = share

    def pd_copies(src, dst, send, recv, name, here, count):
        return [pltpu.make_async_remote_copy(
            src_ref=src, dst_ref=dst.at[here], send_sem=send.at[d], recv_sem=recv.at[here],
            device_id={name: lax.rem(here + d, count)}, device_id_type=MESH)
            for d in range(1, count)]

    pdz = pd_copies(pd_z.at[n_rows], pd_z, pdz_send, pdz_recv, "rows", z, n_rows)
    pds = pd_copies(pd_own_s, pd_s, pds_send, pds_recv, "sub", s, n_sub)
    pdc = pd_copies(pd_own_c, pd_c, pdc_send, pdc_recv, "cols", x, n_cols)

    def gather(first, count):
        rows = slice(first * z_rows, (first + count) * z_rows)
        for p in range(width // k_part):
            if first == 0:
                load_vec[p].wait()
            at = slice(p * k_part, (p + 1) * k_part)
            got = lax.dot_general(
                hot[rows, :], vec[at, :], (((1,), (1,)), ((), ())),
                preferred_element_type=jnp.float32).astype(jnp.bfloat16)
            own[first:first + count, :, at] = got.reshape(count, z_rows, k_part)

    def send_own(first, count):
        @pl.when(z == n_rows - 1)
        def _():
            for q in range(first, first + count):
                z_copy(own, from_r, zl_send, r_recv, q, -1).start()

        @pl.when(z == 0)
        def _():
            for q in range(first, first + count):
                z_copy(own, from_l, zr_send, l_recv, q, 1).start()

    head = HEAD
    gather(0, head)
    pl.semaphore_wait(barrier, n_rows + n_cols + n_sub - 3)
    send_own(0, head)
    for c in pdz:
        c.start()
    gather(head, z_chunks - head)
    send_own(head, z_chunks - head)

    @pl.when(z == 0)
    def _():
        fwd_r[...] = own[...]

    load_tags.wait()
    load_norms.wait()
    tags = tags_ref[...]
    factor = jnp.zeros(tags.shape, jnp.float32)
    for kind in range(norms_ref.shape[0]):
        factor = jnp.where(tags == kind, norms_ref[kind], factor)
    load_ket.wait()
    for slot in range(slot_count):
        scale = column_of(factor[slot:slot + 1, :])
        for h in range(batch // LANES):
            part = (slot, slice(None), slice(h * LANES, (h + 1) * LANES))
            ket[part] = (ket[part].astype(jnp.float32) * scale).astype(jnp.bfloat16)
    load_targets.wait()
    load_counts.wait()
    used = counts_ref[device]

    def stage_for(band):
        low = (band * column_size + column) * per_device
        chosen = jnp.int32(0)
        for slot in range(slot_count):
            target = targets_ref[slot, device]
            fits = (slot < used) & (target >= low) & (target < low + per_device)
            chosen = jnp.where(fits, jnp.int32(slot), chosen)
        return ket[chosen]

    landed[z] = stage_for(z)
    for d in range(1, n_rows):
        stage[d] = stage_for(lax.rem(z + d, n_rows))

    @pl.when(inner)
    def _():
        for d in range(1, n_rows):
            ket_copy(d).start()

    def pd_total(first, dst, recv, here, count):
        total = first[...]
        for d in range(1, count):
            other = lax.rem(here + d, count)
            arrived(dst.at[other], recv.at[other])
            total = total + dst[other]
        return total

    load_prev.wait()
    prev_t[...] = jnp.transpose(prev[...].astype(jnp.float32))

    tilt = jnp.where(inner, hop_lead * (2 * z - (n_rows - 1)) + hop_bias, 0)
    wait_l = jnp.clip(tilt, 0, z_chunks)
    wait_r = jnp.clip(-tilt, 0, z_chunks)
    lag = jnp.maximum(wait_l, wait_r)
    defer = jnp.where(inner, DEFER, 0)
    reduce_lag = jnp.where(s == 0, REDUCE_LAG[0], REDUCE_LAG[1])
    def chip_rows(g):
        return pl.ds(pl.multiple_of(g * g_rows * n_cols, 8), g_rows * n_cols)

    def group_rows(g):
        return pl.ds(pl.multiple_of(g * g_rows, 8), g_rows)

    def sub_copy(g, d):
        return pltpu.make_async_remote_copy(
            src_ref=sub_out.at[d, chip_rows(g)], dst_ref=sub_in.at[s, chip_rows(g)],
            send_sem=sub_send.at[g, d], recv_sem=sub_recv.at[g, s],
            device_id={"sub": lax.rem(s + d, n_sub)}, device_id_type=MESH)

    def col_copy(g, d):
        return pltpu.make_async_remote_copy(
            src_ref=col_out.at[d, group_rows(g)], dst_ref=col_in.at[x, group_rows(g)],
            send_sem=col_send.at[g, d], recv_sem=col_recv.at[g, x],
            device_id={"cols": lax.rem(x + d, n_cols)}, device_id_type=MESH)

    def block_dot(pivot_rows_t, col, sub):
        at = pl.multiple_of((col * n_sub + sub) * rows_here, LANES)
        return jnp.dot(
            pivot_rows_t, vec[:, pl.ds(at, rows_here)], preferred_element_type=jnp.float32)

    def chip_part(g, c):
        return pl.ds(pl.multiple_of((g * n_cols + c) * g_rows, 8), g_rows)

    def multiply(g):
        chunks = pl.ds(g * per, per)

        @pl.when(z < n_rows - 1)
        def _():
            pivot_t[chunks] = fwd_r[chunks] + from_r[chunks]

        @pl.when(z == n_rows - 1)
        def _():
            pivot_t[chunks] = fwd_r[chunks]

        pt = pivot_t[chunks].reshape(g_rows, width)
        for d in range(1, n_sub):
            for c in range(n_cols):
                sub_out[d, chip_part(g, c)] = block_dot(
                    pt, lax.rem(x + c, n_cols), lax.rem(s + d, n_sub))
            sub_copy(g, d).start()
        for c in range(1, n_cols):
            col_out[c, group_rows(g)] = block_dot(pt, lax.rem(x + c, n_cols), s)
        mine[group_rows(g)] = block_dot(pt, x, s)

    def reduce_chip(g):
        for d in range(1, n_sub):
            other = lax.rem(s + d, n_sub)
            arrived(sub_in.at[other, chip_rows(g)], sub_recv.at[g, other])
        for c in range(1, n_cols):
            total = col_out[c, group_rows(g)]
            for d in range(1, n_sub):
                total = total + sub_in[lax.rem(s + d, n_sub), chip_part(g, c)]
            col_out[c, group_rows(g)] = total
            col_copy(g, c).start()
        total = mine[group_rows(g)]
        for d in range(1, n_sub):
            total = total + sub_in[lax.rem(s + d, n_sub), chip_part(g, 0)]
        mine[group_rows(g)] = total

    def step(t, carry):
        q_l, q_r, q_m = t - wait_l, t - wait_r, t - lag - defer

        @pl.when((z > 0) & (q_l >= 0) & (q_l < z_chunks))
        def _():
            z_copy(fwd_r, from_l, zr_send, l_recv, q_l, 1).wait_recv()
            fwd_r[q_l] = from_l[q_l] + own[q_l]

            @pl.when(z < n_rows - 1)
            def _():
                z_copy(fwd_r, from_l, zr_send, l_recv, q_l, 1).start()

        @pl.when((z < n_rows - 1) & (q_r >= 0) & (q_r < z_chunks))
        def _():
            z_copy(fwd_l, from_r, zl_send, r_recv, q_r, -1).wait_recv()

            @pl.when(z > 0)
            def _():
                fwd_l[q_r] = from_r[q_r] + own[q_r]
                z_copy(fwd_l, from_r, zl_send, r_recv, q_r, -1).start()

        for far in range(1, n_rows):
            low_at = min(KET_LOW[0] + (far - 1) * KET_LOW[1], z_chunks - 1)
            high_at = min(KET_HIGH[0] + (far - 1) * KET_HIGH[1], z_chunks - 1)

            @pl.when((z == 0) & (t == low_at))
            def _():
                ket_copy(far).start()

            @pl.when((z == n_rows - 1) & (t == high_at))
            def _():
                ket_copy(n_rows - far).start()

        @pl.when((q_m >= 0) & (lax.rem(q_m, per) == per - 1))
        def _():
            multiply(q_m // per)

        q_e = q_m - reduce_lag + 1

        @pl.when((q_e >= per) & (q_m < z_chunks - 1) & (lax.rem(q_e, per) == 0))
        def _():
            reduce_chip(q_e // per - 1)

        @pl.when(t == PD_SUB)
        def _():
            pd_own_s[...] = pd_total(pd_z.at[n_rows], pd_z, pdz_recv, z, n_rows)
            for c in pds:
                c.start()

        @pl.when(t == PD_COLS)
        def _():
            pd_own_c[...] = pd_total(pd_own_s, pd_s, pds_recv, s, n_sub)
            for c in pdc:
                c.start()

        return carry

    lax.fori_loop(0, z_chunks + lag + defer, step, 0)

    def reduce_rest(g, carry):
        reduce_chip(g)
        return carry

    lax.fori_loop((z_chunks - 1 - reduce_lag) // per, groups, reduce_rest, 0)

    pivot_diag = pd_total(pd_own_c, pd_c, pdc_recv, x, n_cols)
    inverse[...] = 1.0 / jnp.sqrt(column_of(pivot_diag[0:1, :]))
    def each(count, wait):
        def one(q, carry):
            wait(q)
            return carry

        lax.fori_loop(0, count, one, 0)

    def finish(g, total_sq):
        total = mine[group_rows(g)]
        for c in range(1, n_cols):
            other = lax.rem(x + c, n_cols)
            arrived(col_in.at[other, group_rows(g)], col_recv.at[g, other])
            total = total + col_in[other, group_rows(g)]
        rows = group_rows(g)
        scale = inverse[rows, :]
        for h in range(rows_here // LANES):
            cut = slice(h * LANES, (h + 1) * LANES)
            scaled_t[rows, cut] = (prev_t[rows, cut] - total[:, cut]) * scale
        scaled = scaled_t[rows, :]
        return total_sq + jnp.sum(scaled * scaled, axis=0, keepdims=True)

    def write(first, count):
        done = slice(first, first + count)
        new_ref[:, done] = jnp.transpose(scaled_t[done, :]).astype(jnp.bfloat16)

    total_sq = jnp.zeros((1, rows_here), jnp.float32)
    early = (batch - 1) // LANES * LANES // g_rows
    total_sq = lax.fori_loop(0, early, finish, total_sq)
    if early:
        write(0, early * g_rows)
    total_sq = lax.fori_loop(early, last, finish, total_sq)

    for d in range(1, n_rows):
        other = lax.rem(z + d, n_rows)
        arrived(landed.at[other], ket_recv.at[other])
    for place in range(per_device):
        block = device * per_device + place
        source = jnp.int32(0)
        for band in range(n_rows):
            owner = band * column_size + column
            for slot in range(slot_count):
                fits = (slot < counts_ref[owner]) & (targets_ref[slot, owner] == block)
                source = jnp.where(fits, jnp.int32(band), source)
        next_ref[place * block_rows:(place + 1) * block_rows, :] = landed[source]

    for c in pdz + pds + pdc:
        c.wait_send()
    for d in range(1, n_rows):
        ket_copy(d).wait_send()

    @pl.when(z < n_rows - 1)
    def _():
        each(z_chunks, lambda q: z_copy(own, from_l, zr_send, l_recv, q, 1).wait_send())

    @pl.when(z > 0)
    def _():
        each(z_chunks, lambda q: z_copy(own, from_r, zl_send, r_recv, q, -1).wait_send())

    for d in range(1, n_sub):
        each(groups, lambda g: sub_copy(g, d).wait_send())
    for c in range(1, n_cols):
        each(last, lambda g: col_copy(g, c).wait_send())

    total_sq = finish(last, total_sq)
    write(early * g_rows, batch - early * g_rows)
    diag_out_ref[...] = diag_ref[...] - total_sq
    for c in range(1, n_cols):
        col_copy(last, c).wait_send()


def flush(new_ref, diag_ref, next_ref, new_hbm, diag_hbm, next_hbm, sem):
    copies = [
        pltpu.make_async_copy(new_ref, new_hbm, sem.at[0]),
        pltpu.make_async_copy(next_ref, next_hbm, sem.at[1]),
        pltpu.make_async_copy(diag_ref, diag_hbm, sem.at[2]),
    ]
    for c in copies:
        c.start()
    for c in copies:
        c.wait()


def body(mesh_sizes, vectors, previous, pivots, diagonal, ket_blocks, tags, targets, counts, norms):
    n_rows, n_cols, n_sub = mesh_sizes
    width, band_rows = vectors.shape
    rows_here, batch = previous.shape
    slot_count, block_rows, _ = ket_blocks.shape
    z_chunks, hop_lead, hop_bias = 16, 6, 1
    z_rows, m_chunks = batch // z_chunks, z_chunks // PER
    f32, bf16, dma = jnp.float32, jnp.bfloat16, pltpu.SemaphoreType.DMA
    line = pltpu.VMEM((z_chunks, z_rows, width), bf16)
    small = pltpu.VMEM((1, batch), f32)
    scratch = [
        pltpu.VMEM((1, batch), jnp.int32), pltpu.VMEM((1, rows_here), f32),
        pltpu.VMEM(tags.shape, jnp.int32), pltpu.SMEM(targets.shape[::-1], jnp.int32),
        pltpu.SMEM(counts.shape, jnp.int32), pltpu.SMEM(norms.shape, f32),
        pltpu.VMEM(vectors.shape, bf16), pltpu.VMEM(previous.shape, bf16),
        pltpu.VMEM(ket_blocks.shape, bf16), pltpu.VMEM((batch, band_rows), bf16),
        line, line, line, line, line, line,
        pltpu.VMEM((batch, rows_here), f32),
        pltpu.VMEM((n_sub, n_cols * batch, rows_here), f32),
        pltpu.VMEM((n_sub, n_cols * batch, rows_here), f32),
        pltpu.VMEM((batch, rows_here), f32),
        pltpu.VMEM((n_cols, batch, rows_here), f32),
        pltpu.VMEM((n_cols, batch, rows_here), f32),
        pltpu.VMEM((batch, rows_here), f32), pltpu.VMEM((batch, LANES), f32),
        pltpu.VMEM((n_rows, block_rows, batch), bf16),
        pltpu.VMEM((n_rows, block_rows, batch), bf16),
        pltpu.VMEM((n_rows + 1, 1, batch), f32), pltpu.VMEM((n_sub, 1, batch), f32),
        pltpu.VMEM((n_cols, 1, batch), f32), small, small,
        dma((8,)), dma((max(width // PART, 1),)), dma((z_chunks,)), dma((z_chunks,)), dma((z_chunks,)), dma((z_chunks,)),
        dma((m_chunks, n_sub)), dma((m_chunks, n_sub)),
        dma((m_chunks, n_cols)), dma((m_chunks, n_cols)),
        dma((n_rows,)), dma((n_rows,)), dma((n_rows,)), dma((n_rows,)),
        dma((n_sub,)), dma((n_sub,)), dma((n_cols,)), dma((n_cols,)),
    ]
    hbm = pl.BlockSpec(memory_space=pl.ANY)
    vmem = pl.BlockSpec(memory_space=pltpu.VMEM)
    new_vectors, diag_out, next_columns = pl.pallas_call(
        functools.partial(kernel, (n_rows, n_cols, n_sub, hop_lead, hop_bias, PER)),
        out_shape=(
            pltpu.VMEM((rows_here, batch), bf16),
            pltpu.VMEM((1, rows_here), f32),
            pltpu.VMEM((rows_here, batch), bf16),
        ),
        in_specs=[hbm] * 9,
        out_specs=(vmem, vmem, vmem),
        scratch_shapes=scratch,
        compiler_params=pltpu.CompilerParams(
            collective_id=0, has_side_effects=True, vmem_limit_bytes=63 * 1024 * 1024),
    )(
        vectors, previous, pivots.reshape(1, batch), diagonal.reshape(1, rows_here),
        ket_blocks, tags, targets.T, counts, norms,
    )
    new_vectors, diag_out, next_columns = pl.pallas_call(
        flush,
        out_shape=(
            jax.ShapeDtypeStruct((rows_here, batch), bf16),
            jax.ShapeDtypeStruct((1, rows_here), f32),
            jax.ShapeDtypeStruct((rows_here, batch), bf16),
        ),
        in_specs=[vmem] * 3,
        out_specs=(hbm, hbm, hbm),
        scratch_shapes=[dma((3,))],
        compiler_params=pltpu.CompilerParams(vmem_limit_bytes=1024 * 1024),
    )(new_vectors, diag_out, next_columns)
    return new_vectors, diag_out.reshape(rows_here), next_columns


def solution(mesh):
    sizes = tuple(mesh.shape[name] for name in ("rows", "cols", "sub"))
    return jax.shard_map(
        functools.partial(body, sizes),
        mesh=mesh,
        in_specs=(
            P(("cols", "sub"), ("groups", "rows")),
            P(("groups", "rows", "cols", "sub"), None),
            P("groups"),
            P(("groups", "rows", "cols", "sub")),
            P(("groups", "rows", "cols", "sub"), None, None),
            P(("groups", "rows", "cols", "sub"), None),
            P("groups", None),
            P("groups"),
            P(),
        ),
        out_specs=(
            P(("groups", "rows", "cols", "sub"), None),
            P(("groups", "rows", "cols", "sub")),
            P(("groups", "rows", "cols", "sub"), None),
        ),
        check_vma=False,
    )
```

```python
import functools

import jax
import jax.numpy as jnp
from jax import lax
from jax.experimental import pallas as pl
from jax.experimental.pallas import tpu as pltpu
from jax.sharding import PartitionSpec as P

MESH = pl.DeviceIdType.MESH
LANES = 128
PART = 256
KET_LOW, KET_HIGH = (0, 2), (4, 3)
REDUCE_LAG = (1, 5)
HEAD = 2
DEFER = 4
PER = 2
PD_SUB, PD_COLS = 4, 8


def column_of(row):
    return jnp.transpose(jnp.broadcast_to(row, (LANES, row.shape[1])))


def kernel(
    sizes,
    vec_hbm, prev_hbm, piv_hbm, diag_hbm, ket_hbm, tags_hbm, targets_hbm, counts_hbm, norms_hbm,
    new_ref, diag_out_ref, next_ref,
    piv_ref, diag_ref, tags_ref, targets_ref, counts_ref, norms_ref,
    vec, prev, ket, hot, own, fwd_r, fwd_l, from_l, from_r,
    pivot_t, prev_t, sub_out, sub_in, mine, col_out, col_in, scaled_t, inverse,
    stage, landed, pd_z, pd_s, pd_c, pd_own_s, pd_own_c,
    load_sem, vec_sem, zr_send, zl_send, l_recv, r_recv, sub_send, sub_recv, col_send, col_recv,
    ket_send, ket_recv, pdz_send, pdz_recv, pds_send, pds_recv, pdc_send, pdc_recv,
):
    n_rows, n_cols, n_sub, hop_lead, hop_bias, per = sizes
    z, x, s = lax.axis_index("rows"), lax.axis_index("cols"), lax.axis_index("sub")
    column_size = n_cols * n_sub
    column = x * n_sub + s
    device = z * column_size + column
    slot_count, block_rows, batch = ket_hbm.shape
    rows_here = prev_hbm.shape[0]
    per_device = rows_here // block_rows
    width, band_rows = vec_hbm.shape
    z_chunks, z_rows = own.shape[0], own.shape[1]
    groups = z_chunks // per
    last = groups - 1
    g_rows = per * z_rows

    k_part = PART if width % PART == 0 else width
    load_piv = pltpu.make_async_copy(piv_hbm, piv_ref, load_sem.at[0])
    load_piv.start()
    load_diag = pltpu.make_async_copy(diag_hbm, diag_ref, load_sem.at[1])
    load_diag.start()
    load_vec = []
    for p in range(width // k_part):
        at = pl.ds(p * k_part, k_part)
        load_vec.append(pltpu.make_async_copy(vec_hbm.at[at], vec.at[at], vec_sem.at[p]))
        load_vec[-1].start()
    load_ket = pltpu.make_async_copy(ket_hbm, ket, load_sem.at[2])
    load_tags = pltpu.make_async_copy(tags_hbm, tags_ref, load_sem.at[3])
    load_targets = pltpu.make_async_copy(targets_hbm, targets_ref, load_sem.at[4])
    load_counts = pltpu.make_async_copy(counts_hbm, counts_ref, load_sem.at[5])
    load_norms = pltpu.make_async_copy(norms_hbm, norms_ref, load_sem.at[6])
    load_prev = pltpu.make_async_copy(prev_hbm, prev, load_sem.at[7])
    for c in (load_tags, load_norms, load_targets, load_counts):
        c.start()

    barrier = pltpu.get_barrier_semaphore()
    for name, here, count in (("rows", z, n_rows), ("cols", x, n_cols), ("sub", s, n_sub)):
        for d in range(1, count):
            pl.semaphore_signal(
                barrier, inc=1, device_id={name: lax.rem(here + d, count)}, device_id_type=MESH
            )

    load_piv.wait()
    piv_col = column_of(piv_ref[...].astype(jnp.float32)).astype(jnp.int32) - z * band_rows
    lane = lax.broadcasted_iota(jnp.int32, (batch, LANES), 1)
    for t in range(band_rows // LANES):
        hot[:, t * LANES:(t + 1) * LANES] = (piv_col == lane + t * LANES).astype(
            jnp.float32).astype(jnp.bfloat16)

    def ket_copy(d):
        return pltpu.make_async_remote_copy(
            src_ref=stage.at[d], dst_ref=landed.at[z], send_sem=ket_send.at[d],
            recv_sem=ket_recv.at[z], device_id={"rows": lax.rem(z + d, n_rows)},
            device_id_type=MESH)

    inner = (z > 0) & (z < n_rows - 1)

    def z_copy(src, dst, send, recv, q, dz):
        return pltpu.make_async_remote_copy(
            src_ref=src.at[q], dst_ref=dst.at[q], send_sem=send.at[q], recv_sem=recv.at[q],
            device_id={"rows": lax.rem(z + dz + n_rows, n_rows)}, device_id_type=MESH)

    def arrived(dst, sem):
        pltpu.make_async_remote_copy(
            src_ref=dst, dst_ref=dst, send_sem=sem, recv_sem=sem,
            device_id={"sub": lax.rem(s + 1, n_sub)}, device_id_type=MESH).wait_recv()

    load_diag.wait()
    diag_col = column_of(diag_ref[...])
    row = lax.broadcasted_iota(jnp.int32, (rows_here, LANES), 0) + device * rows_here
    for h in range(batch // LANES):
        cut = slice(h * LANES, (h + 1) * LANES)
        share = jnp.sum(jnp.where(piv_ref[:, cut] == row, diag_col, 0.0), axis=0, keepdims=True)
        pd_z[n_rows, :, cut] = share

    def pd_copies(src, dst, send, recv, name, here, count):
        return [pltpu.make_async_remote_copy(
            src_ref=src, dst_ref=dst.at[here], send_sem=send.at[d], recv_sem=recv.at[here],
            device_id={name: lax.rem(here + d, count)}, device_id_type=MESH)
            for d in range(1, count)]

    pdz = pd_copies(pd_z.at[n_rows], pd_z, pdz_send, pdz_recv, "rows", z, n_rows)
    pds = pd_copies(pd_own_s, pd_s, pds_send, pds_recv, "sub", s, n_sub)
    pdc = pd_copies(pd_own_c, pd_c, pdc_send, pdc_recv, "cols", x, n_cols)

    def gather(first, count):
        rows = slice(first * z_rows, (first + count) * z_rows)
        for p in range(width // k_part):
            if first == 0:
                load_vec[p].wait()
            at = slice(p * k_part, (p + 1) * k_part)
            got = lax.dot_general(
                hot[rows, :], vec[at, :], (((1,), (1,)), ((), ())),
                preferred_element_type=jnp.float32).astype(jnp.bfloat16)
            own[first:first + count, :, at] = got.reshape(count, z_rows, k_part)

    def send_own(first, count):
        @pl.when(z == n_rows - 1)
        def _():
            for q in range(first, first + count):
                z_copy(own, from_r, zl_send, r_recv, q, -1).start()

        @pl.when(z == 0)
        def _():
            for q in range(first, first + count):
                z_copy(own, from_l, zr_send, l_recv, q, 1).start()

    head = HEAD
    gather(0, head)
    load_ket.start()
    load_prev.start()
    pl.semaphore_wait(barrier, n_rows + n_cols + n_sub - 3)
    send_own(0, head)
    gather(head, z_chunks - head)
    for c in pdz:
        c.start()
    send_own(head, z_chunks - head)

    @pl.when(z == 0)
    def _():
        fwd_r[...] = own[...]

    load_tags.wait()
    load_norms.wait()
    tags = tags_ref[...]
    factor = jnp.zeros(tags.shape, jnp.float32)
    for kind in range(norms_ref.shape[0]):
        factor = jnp.where(tags == kind, norms_ref[kind], factor)
    load_ket.wait()
    for slot in range(slot_count):
        scale = column_of(factor[slot:slot + 1, :])
        for h in range(batch // LANES):
            part = (slot, slice(None), slice(h * LANES, (h + 1) * LANES))
            ket[part] = (ket[part].astype(jnp.float32) * scale).astype(jnp.bfloat16)
    load_targets.wait()
    load_counts.wait()
    used = counts_ref[device]

    def stage_for(band):
        low = (band * column_size + column) * per_device
        chosen = jnp.int32(0)
        for slot in range(slot_count):
            target = targets_ref[slot, device]
            fits = (slot < used) & (target >= low) & (target < low + per_device)
            chosen = jnp.where(fits, jnp.int32(slot), chosen)
        return ket[chosen]

    landed[z] = stage_for(z)
    for d in range(1, n_rows):
        stage[d] = stage_for(lax.rem(z + d, n_rows))

    @pl.when(inner)
    def _():
        for d in range(1, n_rows):
            ket_copy(d).start()

    def pd_total(first, dst, recv, here, count):
        total = first[...]
        for d in range(1, count):
            other = lax.rem(here + d, count)
            arrived(dst.at[other], recv.at[other])
            total = total + dst[other]
        return total

    load_prev.wait()
    prev_t[...] = jnp.transpose(prev[...].astype(jnp.float32))

    lead = jnp.where(s == 0, hop_lead[0], hop_lead[1])
    tilt = jnp.where(inner, lead * (2 * z - (n_rows - 1)) + hop_bias, 0)
    wait_l = jnp.clip(tilt, 0, z_chunks)
    wait_r = jnp.clip(-tilt, 0, z_chunks)
    lag = jnp.maximum(wait_l, wait_r)
    defer = jnp.where(inner, DEFER, 0)
    reduce_lag = jnp.where(s == 0, REDUCE_LAG[0], REDUCE_LAG[1])
    def chip_rows(g):
        return pl.ds(pl.multiple_of(g * g_rows * n_cols, 8), g_rows * n_cols)

    def group_rows(g):
        return pl.ds(pl.multiple_of(g * g_rows, 8), g_rows)

    def sub_copy(g, d):
        return pltpu.make_async_remote_copy(
            src_ref=sub_out.at[d, chip_rows(g)], dst_ref=sub_in.at[s, chip_rows(g)],
            send_sem=sub_send.at[g, d], recv_sem=sub_recv.at[g, s],
            device_id={"sub": lax.rem(s + d, n_sub)}, device_id_type=MESH)

    def col_copy(g, d):
        return pltpu.make_async_remote_copy(
            src_ref=col_out.at[d, group_rows(g)], dst_ref=col_in.at[x, group_rows(g)],
            send_sem=col_send.at[g, d], recv_sem=col_recv.at[g, x],
            device_id={"cols": lax.rem(x + d, n_cols)}, device_id_type=MESH)

    def block_dot(pivot_rows_t, col, sub):
        at = pl.multiple_of((col * n_sub + sub) * rows_here, LANES)
        return jnp.dot(
            pivot_rows_t, vec[:, pl.ds(at, rows_here)], preferred_element_type=jnp.float32)

    def chip_part(g, c):
        return pl.ds(pl.multiple_of((g * n_cols + c) * g_rows, 8), g_rows)

    def multiply(g):
        chunks = pl.ds(g * per, per)

        @pl.when(z < n_rows - 1)
        def _():
            pivot_t[chunks] = fwd_r[chunks] + from_r[chunks]

        @pl.when(z == n_rows - 1)
        def _():
            pivot_t[chunks] = fwd_r[chunks]

        pt = pivot_t[chunks].reshape(g_rows, width)
        for d in range(1, n_sub):
            for c in range(n_cols):
                sub_out[d, chip_part(g, c)] = block_dot(
                    pt, lax.rem(x + c, n_cols), lax.rem(s + d, n_sub))
            sub_copy(g, d).start()
        for c in range(1, n_cols):
            col_out[c, group_rows(g)] = block_dot(pt, lax.rem(x + c, n_cols), s)
        mine[group_rows(g)] = block_dot(pt, x, s)

    def reduce_chip(g):
        for d in range(1, n_sub):
            other = lax.rem(s + d, n_sub)
            arrived(sub_in.at[other, chip_rows(g)], sub_recv.at[g, other])
        for c in range(1, n_cols):
            total = col_out[c, group_rows(g)]
            for d in range(1, n_sub):
                total = total + sub_in[lax.rem(s + d, n_sub), chip_part(g, c)]
            col_out[c, group_rows(g)] = total
            col_copy(g, c).start()
        total = mine[group_rows(g)]
        for d in range(1, n_sub):
            total = total + sub_in[lax.rem(s + d, n_sub), chip_part(g, 0)]
        mine[group_rows(g)] = total

    def step(t, carry):
        q_l, q_r, q_m = t - wait_l, t - wait_r, t - lag - defer

        @pl.when((z > 0) & (q_l >= 0) & (q_l < z_chunks))
        def _():
            z_copy(fwd_r, from_l, zr_send, l_recv, q_l, 1).wait_recv()
            fwd_r[q_l] = from_l[q_l] + own[q_l]

            @pl.when(z < n_rows - 1)
            def _():
                z_copy(fwd_r, from_l, zr_send, l_recv, q_l, 1).start()

        @pl.when((z < n_rows - 1) & (q_r >= 0) & (q_r < z_chunks))
        def _():
            z_copy(fwd_l, from_r, zl_send, r_recv, q_r, -1).wait_recv()

            @pl.when(z > 0)
            def _():
                fwd_l[q_r] = from_r[q_r] + own[q_r]
                z_copy(fwd_l, from_r, zl_send, r_recv, q_r, -1).start()

        for far in range(1, n_rows):
            low_at = min(KET_LOW[0] + (far - 1) * KET_LOW[1], z_chunks - 1)
            high_at = min(KET_HIGH[0] + (far - 1) * KET_HIGH[1], z_chunks - 1)

            @pl.when((z == 0) & (t == low_at))
            def _():
                ket_copy(far).start()

            @pl.when((z == n_rows - 1) & (t == high_at))
            def _():
                ket_copy(n_rows - far).start()

        @pl.when((q_m >= 0) & (lax.rem(q_m, per) == per - 1))
        def _():
            multiply(q_m // per)

        q_e = q_m - reduce_lag + 1

        @pl.when((q_e >= per) & (q_m < z_chunks - 1) & (lax.rem(q_e, per) == 0))
        def _():
            reduce_chip(q_e // per - 1)

        @pl.when(t == PD_SUB)
        def _():
            pd_own_s[...] = pd_total(pd_z.at[n_rows], pd_z, pdz_recv, z, n_rows)
            for c in pds:
                c.start()

        @pl.when(t == PD_COLS)
        def _():
            pd_own_c[...] = pd_total(pd_own_s, pd_s, pds_recv, s, n_sub)
            for c in pdc:
                c.start()

        return carry

    lax.fori_loop(0, z_chunks + lag + defer, step, 0)

    def reduce_rest(g, carry):
        reduce_chip(g)
        return carry

    lax.fori_loop((z_chunks - 1 - reduce_lag) // per, groups, reduce_rest, 0)

    pivot_diag = pd_total(pd_own_c, pd_c, pdc_recv, x, n_cols)
    inverse[...] = 1.0 / jnp.sqrt(column_of(pivot_diag[0:1, :]))
    def each(count, wait):
        def one(q, carry):
            wait(q)
            return carry

        lax.fori_loop(0, count, one, 0)

    def finish(g, total_sq):
        total = mine[group_rows(g)]
        for c in range(1, n_cols):
            other = lax.rem(x + c, n_cols)
            arrived(col_in.at[other, group_rows(g)], col_recv.at[g, other])
            total = total + col_in[other, group_rows(g)]
        rows = group_rows(g)
        scale = inverse[rows, :]
        for h in range(rows_here // LANES):
            cut = slice(h * LANES, (h + 1) * LANES)
            scaled_t[rows, cut] = (prev_t[rows, cut] - total[:, cut]) * scale
        scaled = scaled_t[rows, :]
        return total_sq + jnp.sum(scaled * scaled, axis=0, keepdims=True)

    def write(first, count):
        done = slice(first, first + count)
        new_ref[:, done] = jnp.transpose(scaled_t[done, :]).astype(jnp.bfloat16)

    total_sq = jnp.zeros((1, rows_here), jnp.float32)
    early = (batch - 1) // LANES * LANES // g_rows
    total_sq = lax.fori_loop(0, early, finish, total_sq)
    if early:
        write(0, early * g_rows)
    total_sq = lax.fori_loop(early, last, finish, total_sq)

    for d in range(1, n_rows):
        other = lax.rem(z + d, n_rows)
        arrived(landed.at[other], ket_recv.at[other])
    for place in range(per_device):
        block = device * per_device + place
        source = jnp.int32(0)
        for band in range(n_rows):
            owner = band * column_size + column
            for slot in range(slot_count):
                fits = (slot < counts_ref[owner]) & (targets_ref[slot, owner] == block)
                source = jnp.where(fits, jnp.int32(band), source)
        next_ref[place * block_rows:(place + 1) * block_rows, :] = landed[source]

    for c in pdz + pds + pdc:
        c.wait_send()
    for d in range(1, n_rows):
        ket_copy(d).wait_send()

    @pl.when(z < n_rows - 1)
    def _():
        each(z_chunks, lambda q: z_copy(own, from_l, zr_send, l_recv, q, 1).wait_send())

    @pl.when(z > 0)
    def _():
        each(z_chunks, lambda q: z_copy(own, from_r, zl_send, r_recv, q, -1).wait_send())

    for d in range(1, n_sub):
        each(groups, lambda g: sub_copy(g, d).wait_send())
    for c in range(1, n_cols):
        each(last, lambda g: col_copy(g, c).wait_send())

    total_sq = finish(last, total_sq)
    write(early * g_rows, batch - early * g_rows)
    diag_out_ref[...] = diag_ref[...] - total_sq
    for c in range(1, n_cols):
        col_copy(last, c).wait_send()


def flush(new_ref, diag_ref, next_ref, new_hbm, diag_hbm, next_hbm, sem):
    copies = [
        pltpu.make_async_copy(new_ref, new_hbm, sem.at[0]),
        pltpu.make_async_copy(next_ref, next_hbm, sem.at[1]),
        pltpu.make_async_copy(diag_ref, diag_hbm, sem.at[2]),
    ]
    for c in copies:
        c.start()
    for c in copies:
        c.wait()


def body(mesh_sizes, vectors, previous, pivots, diagonal, ket_blocks, tags, targets, counts, norms):
    n_rows, n_cols, n_sub = mesh_sizes
    width, band_rows = vectors.shape
    rows_here, batch = previous.shape
    slot_count, block_rows, _ = ket_blocks.shape
    z_chunks, hop_lead, hop_bias = 16, (7, 5), 1
    z_rows, m_chunks = batch // z_chunks, z_chunks // PER
    f32, bf16, dma = jnp.float32, jnp.bfloat16, pltpu.SemaphoreType.DMA
    line = pltpu.VMEM((z_chunks, z_rows, width), bf16)
    small = pltpu.VMEM((1, batch), f32)
    scratch = [
        pltpu.VMEM((1, batch), jnp.int32), pltpu.VMEM((1, rows_here), f32),
        pltpu.VMEM(tags.shape, jnp.int32), pltpu.SMEM(targets.shape[::-1], jnp.int32),
        pltpu.SMEM(counts.shape, jnp.int32), pltpu.SMEM(norms.shape, f32),
        pltpu.VMEM(vectors.shape, bf16), pltpu.VMEM(previous.shape, bf16),
        pltpu.VMEM(ket_blocks.shape, bf16), pltpu.VMEM((batch, band_rows), bf16),
        line, line, line, line, line, line,
        pltpu.VMEM((batch, rows_here), f32),
        pltpu.VMEM((n_sub, n_cols * batch, rows_here), f32),
        pltpu.VMEM((n_sub, n_cols * batch, rows_here), f32),
        pltpu.VMEM((batch, rows_here), f32),
        pltpu.VMEM((n_cols, batch, rows_here), f32),
        pltpu.VMEM((n_cols, batch, rows_here), f32),
        pltpu.VMEM((batch, rows_here), f32), pltpu.VMEM((batch, LANES), f32),
        pltpu.VMEM((n_rows, block_rows, batch), bf16),
        pltpu.VMEM((n_rows, block_rows, batch), bf16),
        pltpu.VMEM((n_rows + 1, 1, batch), f32), pltpu.VMEM((n_sub, 1, batch), f32),
        pltpu.VMEM((n_cols, 1, batch), f32), small, small,
        dma((8,)), dma((max(width // PART, 1),)), dma((z_chunks,)), dma((z_chunks,)), dma((z_chunks,)), dma((z_chunks,)),
        dma((m_chunks, n_sub)), dma((m_chunks, n_sub)),
        dma((m_chunks, n_cols)), dma((m_chunks, n_cols)),
        dma((n_rows,)), dma((n_rows,)), dma((n_rows,)), dma((n_rows,)),
        dma((n_sub,)), dma((n_sub,)), dma((n_cols,)), dma((n_cols,)),
    ]
    hbm = pl.BlockSpec(memory_space=pl.ANY)
    vmem = pl.BlockSpec(memory_space=pltpu.VMEM)
    new_vectors, diag_out, next_columns = pl.pallas_call(
        functools.partial(kernel, (n_rows, n_cols, n_sub, hop_lead, hop_bias, PER)),
        out_shape=(
            pltpu.VMEM((rows_here, batch), bf16),
            pltpu.VMEM((1, rows_here), f32),
            pltpu.VMEM((rows_here, batch), bf16),
        ),
        in_specs=[hbm] * 9,
        out_specs=(vmem, vmem, vmem),
        scratch_shapes=scratch,
        compiler_params=pltpu.CompilerParams(
            collective_id=0, has_side_effects=True, vmem_limit_bytes=63 * 1024 * 1024),
    )(
        vectors, previous, pivots.reshape(1, batch), diagonal.reshape(1, rows_here),
        ket_blocks, tags, targets.T, counts, norms,
    )
    new_vectors, diag_out, next_columns = pl.pallas_call(
        flush,
        out_shape=(
            jax.ShapeDtypeStruct((rows_here, batch), bf16),
            jax.ShapeDtypeStruct((1, rows_here), f32),
            jax.ShapeDtypeStruct((rows_here, batch), bf16),
        ),
        in_specs=[vmem] * 3,
        out_specs=(hbm, hbm, hbm),
        scratch_shapes=[dma((3,))],
        compiler_params=pltpu.CompilerParams(vmem_limit_bytes=1024 * 1024),
    )(new_vectors, diag_out, next_columns)
    return new_vectors, diag_out.reshape(rows_here), next_columns


def solution(mesh):
    sizes = tuple(mesh.shape[name] for name in ("rows", "cols", "sub"))
    return jax.shard_map(
        functools.partial(body, sizes),
        mesh=mesh,
        in_specs=(
            P(("cols", "sub"), ("groups", "rows")),
            P(("groups", "rows", "cols", "sub"), None),
            P("groups"),
            P(("groups", "rows", "cols", "sub")),
            P(("groups", "rows", "cols", "sub"), None, None),
            P(("groups", "rows", "cols", "sub"), None),
            P("groups", None),
            P("groups"),
            P(),
        ),
        out_specs=(
            P(("groups", "rows", "cols", "sub"), None),
            P(("groups", "rows", "cols", "sub")),
            P(("groups", "rows", "cols", "sub"), None),
        ),
        check_vma=False,
    )
```

```python
import functools

import jax
import jax.numpy as jnp
from jax import lax
from jax.experimental import pallas as pl
from jax.experimental.pallas import tpu as pltpu
from jax.sharding import PartitionSpec as P

MESH = pl.DeviceIdType.MESH
LANES = 128
PART = 256
KET_LOW, KET_HIGH = (0, 2), (4, 3)
REDUCE_LAG = (1, 5)
HEAD = 2
DEFER = 4
PER = 2
PD_SUB, PD_COLS = 4, 8


def column_of(row):
    return jnp.transpose(jnp.broadcast_to(row, (LANES, row.shape[1])))


def kernel(
    sizes,
    vec_hbm, prev_hbm, piv_hbm, diag_hbm, ket_hbm, tags_hbm, targets_hbm, counts_hbm, norms_hbm,
    new_ref, diag_out_ref, next_ref,
    piv_ref, diag_ref, tags_ref, targets_ref, counts_ref, norms_ref,
    vec, prev, ket, hot, own, fwd_r, fwd_l, from_l, from_r,
    pivot_t, prev_t, sub_out, sub_in, mine, col_out, col_in, scaled_t, inverse,
    stage, landed, pd_z, pd_s, pd_c, pd_own_s, pd_own_c,
    load_sem, vec_sem, zr_send, zl_send, l_recv, r_recv, sub_send, sub_recv, col_send, col_recv,
    ket_send, ket_recv, pdz_send, pdz_recv, pds_send, pds_recv, pdc_send, pdc_recv,
):
    n_rows, n_cols, n_sub, hop_lead, hop_bias, per = sizes
    z, x, s = lax.axis_index("rows"), lax.axis_index("cols"), lax.axis_index("sub")
    column_size = n_cols * n_sub
    column = x * n_sub + s
    device = z * column_size + column
    slot_count, block_rows, batch = ket_hbm.shape
    rows_here = prev_hbm.shape[0]
    per_device = rows_here // block_rows
    width, band_rows = vec_hbm.shape
    z_chunks, z_rows = own.shape[0], own.shape[1]
    groups = z_chunks // per
    last = groups - 1
    g_rows = per * z_rows

    k_part = PART if width % PART == 0 else width
    load_piv = pltpu.make_async_copy(piv_hbm, piv_ref, load_sem.at[0])
    load_piv.start()
    load_diag = pltpu.make_async_copy(diag_hbm, diag_ref, load_sem.at[1])
    load_diag.start()
    load_vec = []
    load_vec.append(pltpu.make_async_copy(vec_hbm, vec, vec_sem.at[0]))
    load_vec[-1].start()
    load_ket = pltpu.make_async_copy(ket_hbm, ket, load_sem.at[2])
    load_tags = pltpu.make_async_copy(tags_hbm, tags_ref, load_sem.at[3])
    load_targets = pltpu.make_async_copy(targets_hbm, targets_ref, load_sem.at[4])
    load_counts = pltpu.make_async_copy(counts_hbm, counts_ref, load_sem.at[5])
    load_norms = pltpu.make_async_copy(norms_hbm, norms_ref, load_sem.at[6])
    load_prev = pltpu.make_async_copy(prev_hbm, prev, load_sem.at[7])
    for c in (load_tags, load_norms, load_targets, load_counts):
        c.start()

    barrier = pltpu.get_barrier_semaphore()
    for name, here, count in (("rows", z, n_rows), ("cols", x, n_cols), ("sub", s, n_sub)):
        for d in range(1, count):
            pl.semaphore_signal(
                barrier, inc=1, device_id={name: lax.rem(here + d, count)}, device_id_type=MESH
            )

    load_piv.wait()
    piv_col = column_of(piv_ref[...].astype(jnp.float32)).astype(jnp.int32) - z * band_rows
    lane = lax.broadcasted_iota(jnp.int32, (batch, LANES), 1)
    for t in range(band_rows // LANES):
        hot[:, t * LANES:(t + 1) * LANES] = (piv_col == lane + t * LANES).astype(
            jnp.float32).astype(jnp.bfloat16)

    def ket_copy(d):
        return pltpu.make_async_remote_copy(
            src_ref=stage.at[d], dst_ref=landed.at[z], send_sem=ket_send.at[d],
            recv_sem=ket_recv.at[z], device_id={"rows": lax.rem(z + d, n_rows)},
            device_id_type=MESH)

    inner = (z > 0) & (z < n_rows - 1)

    def z_copy(src, dst, send, recv, q, dz):
        return pltpu.make_async_remote_copy(
            src_ref=src.at[q], dst_ref=dst.at[q], send_sem=send.at[q], recv_sem=recv.at[q],
            device_id={"rows": lax.rem(z + dz + n_rows, n_rows)}, device_id_type=MESH)

    def arrived(dst, sem):
        pltpu.make_async_remote_copy(
            src_ref=dst, dst_ref=dst, send_sem=sem, recv_sem=sem,
            device_id={"sub": lax.rem(s + 1, n_sub)}, device_id_type=MESH).wait_recv()

    load_diag.wait()
    diag_col = column_of(diag_ref[...])
    row = lax.broadcasted_iota(jnp.int32, (rows_here, LANES), 0) + device * rows_here
    for h in range(batch // LANES):
        cut = slice(h * LANES, (h + 1) * LANES)
        share = jnp.sum(jnp.where(piv_ref[:, cut] == row, diag_col, 0.0), axis=0, keepdims=True)
        pd_z[n_rows, :, cut] = share

    def pd_copies(src, dst, send, recv, name, here, count):
        return [pltpu.make_async_remote_copy(
            src_ref=src, dst_ref=dst.at[here], send_sem=send.at[d], recv_sem=recv.at[here],
            device_id={name: lax.rem(here + d, count)}, device_id_type=MESH)
            for d in range(1, count)]

    pdz = pd_copies(pd_z.at[n_rows], pd_z, pdz_send, pdz_recv, "rows", z, n_rows)
    pds = pd_copies(pd_own_s, pd_s, pds_send, pds_recv, "sub", s, n_sub)
    pdc = pd_copies(pd_own_c, pd_c, pdc_send, pdc_recv, "cols", x, n_cols)

    def gather(first, count):
        rows = slice(first * z_rows, (first + count) * z_rows)
        for p in range(width // k_part):
            if first == 0 and p == 0:
                load_vec[p].wait()
            at = slice(p * k_part, (p + 1) * k_part)
            got = lax.dot_general(
                hot[rows, :], vec[at, :], (((1,), (1,)), ((), ())),
                preferred_element_type=jnp.float32).astype(jnp.bfloat16)
            own[first:first + count, :, at] = got.reshape(count, z_rows, k_part)

    def send_own(first, count):
        @pl.when(z == n_rows - 1)
        def _():
            for q in range(first, first + count):
                z_copy(own, from_r, zl_send, r_recv, q, -1).start()

        @pl.when(z == 0)
        def _():
            for q in range(first, first + count):
                z_copy(own, from_l, zr_send, l_recv, q, 1).start()

    head = HEAD
    gather(0, head)
    load_ket.start()
    load_prev.start()
    pl.semaphore_wait(barrier, n_rows + n_cols + n_sub - 3)
    send_own(0, head)
    gather(head, z_chunks - head)
    for c in pdz:
        c.start()
    send_own(head, z_chunks - head)

    @pl.when(z == 0)
    def _():
        fwd_r[...] = own[...]

    load_tags.wait()
    load_norms.wait()
    tags = tags_ref[...]
    factor = jnp.zeros(tags.shape, jnp.float32)
    for kind in range(norms_ref.shape[0]):
        factor = jnp.where(tags == kind, norms_ref[kind], factor)
    load_ket.wait()
    for slot in range(slot_count):
        scale = column_of(factor[slot:slot + 1, :])
        for h in range(batch // LANES):
            part = (slot, slice(None), slice(h * LANES, (h + 1) * LANES))
            ket[part] = (ket[part].astype(jnp.float32) * scale).astype(jnp.bfloat16)
    load_targets.wait()
    load_counts.wait()
    used = counts_ref[device]

    def stage_for(band):
        low = (band * column_size + column) * per_device
        chosen = jnp.int32(0)
        for slot in range(slot_count):
            target = targets_ref[slot, device]
            fits = (slot < used) & (target >= low) & (target < low + per_device)
            chosen = jnp.where(fits, jnp.int32(slot), chosen)
        return ket[chosen]

    landed[z] = stage_for(z)
    for d in range(1, n_rows):
        stage[d] = stage_for(lax.rem(z + d, n_rows))

    @pl.when(inner)
    def _():
        for d in range(1, n_rows):
            ket_copy(d).start()

    def pd_total(first, dst, recv, here, count):
        total = first[...]
        for d in range(1, count):
            other = lax.rem(here + d, count)
            arrived(dst.at[other], recv.at[other])
            total = total + dst[other]
        return total

    load_prev.wait()
    prev_t[...] = jnp.transpose(prev[...].astype(jnp.float32))

    lead = jnp.where(s == 0, hop_lead[0], hop_lead[1])
    tilt = jnp.where(inner, lead * (2 * z - (n_rows - 1)) + hop_bias, 0)
    wait_l = jnp.clip(tilt, 0, z_chunks)
    wait_r = jnp.clip(-tilt, 0, z_chunks)
    lag = jnp.maximum(wait_l, wait_r)
    defer = jnp.where(inner, DEFER, 0)
    reduce_lag = jnp.where(s == 0, REDUCE_LAG[0], REDUCE_LAG[1])
    def chip_rows(g):
        return pl.ds(pl.multiple_of(g * g_rows * n_cols, 8), g_rows * n_cols)

    def group_rows(g):
        return pl.ds(pl.multiple_of(g * g_rows, 8), g_rows)

    def sub_copy(g, d):
        return pltpu.make_async_remote_copy(
            src_ref=sub_out.at[d, chip_rows(g)], dst_ref=sub_in.at[s, chip_rows(g)],
            send_sem=sub_send.at[g, d], recv_sem=sub_recv.at[g, s],
            device_id={"sub": lax.rem(s + d, n_sub)}, device_id_type=MESH)

    def col_copy(g, d):
        return pltpu.make_async_remote_copy(
            src_ref=col_out.at[d, group_rows(g)], dst_ref=col_in.at[x, group_rows(g)],
            send_sem=col_send.at[g, d], recv_sem=col_recv.at[g, x],
            device_id={"cols": lax.rem(x + d, n_cols)}, device_id_type=MESH)

    def block_dot(pivot_rows_t, col, sub):
        at = pl.multiple_of((col * n_sub + sub) * rows_here, LANES)
        return jnp.dot(
            pivot_rows_t, vec[:, pl.ds(at, rows_here)], preferred_element_type=jnp.float32)

    def chip_part(g, c):
        return pl.ds(pl.multiple_of((g * n_cols + c) * g_rows, 8), g_rows)

    def multiply(g):
        chunks = pl.ds(g * per, per)

        @pl.when(z < n_rows - 1)
        def _():
            pivot_t[chunks] = fwd_r[chunks] + from_r[chunks]

        @pl.when(z == n_rows - 1)
        def _():
            pivot_t[chunks] = fwd_r[chunks]

        pt = pivot_t[chunks].reshape(g_rows, width)
        for d in range(1, n_sub):
            for c in range(n_cols):
                sub_out[d, chip_part(g, c)] = block_dot(
                    pt, lax.rem(x + c, n_cols), lax.rem(s + d, n_sub))
            sub_copy(g, d).start()
        for c in range(1, n_cols):
            col_out[c, group_rows(g)] = block_dot(pt, lax.rem(x + c, n_cols), s)
        mine[group_rows(g)] = block_dot(pt, x, s)

    def reduce_chip(g):
        for d in range(1, n_sub):
            other = lax.rem(s + d, n_sub)
            arrived(sub_in.at[other, chip_rows(g)], sub_recv.at[g, other])
        for c in range(1, n_cols):
            total = col_out[c, group_rows(g)]
            for d in range(1, n_sub):
                total = total + sub_in[lax.rem(s + d, n_sub), chip_part(g, c)]
            col_out[c, group_rows(g)] = total
            col_copy(g, c).start()
        total = mine[group_rows(g)]
        for d in range(1, n_sub):
            total = total + sub_in[lax.rem(s + d, n_sub), chip_part(g, 0)]
        mine[group_rows(g)] = total

    def step(t, carry):
        q_l, q_r, q_m = t - wait_l, t - wait_r, t - lag - defer

        @pl.when((z > 0) & (q_l >= 0) & (q_l < z_chunks))
        def _():
            z_copy(fwd_r, from_l, zr_send, l_recv, q_l, 1).wait_recv()
            fwd_r[q_l] = from_l[q_l] + own[q_l]

            @pl.when(z < n_rows - 1)
            def _():
                z_copy(fwd_r, from_l, zr_send, l_recv, q_l, 1).start()

        @pl.when((z < n_rows - 1) & (q_r >= 0) & (q_r < z_chunks))
        def _():
            z_copy(fwd_l, from_r, zl_send, r_recv, q_r, -1).wait_recv()

            @pl.when(z > 0)
            def _():
                fwd_l[q_r] = from_r[q_r] + own[q_r]
                z_copy(fwd_l, from_r, zl_send, r_recv, q_r, -1).start()

        for far in range(1, n_rows):
            low_at = min(KET_LOW[0] + (far - 1) * KET_LOW[1], z_chunks - 1)
            high_at = min(KET_HIGH[0] + (far - 1) * KET_HIGH[1], z_chunks - 1)

            @pl.when((z == 0) & (t == low_at))
            def _():
                ket_copy(far).start()

            @pl.when((z == n_rows - 1) & (t == high_at))
            def _():
                ket_copy(n_rows - far).start()

        @pl.when((q_m >= 0) & (lax.rem(q_m, per) == per - 1))
        def _():
            multiply(q_m // per)

        q_e = q_m - reduce_lag + 1

        @pl.when((q_e >= per) & (q_m < z_chunks - 1) & (lax.rem(q_e, per) == 0))
        def _():
            reduce_chip(q_e // per - 1)

        @pl.when(t == PD_SUB)
        def _():
            pd_own_s[...] = pd_total(pd_z.at[n_rows], pd_z, pdz_recv, z, n_rows)
            for c in pds:
                c.start()

        @pl.when(t == PD_COLS)
        def _():
            pd_own_c[...] = pd_total(pd_own_s, pd_s, pds_recv, s, n_sub)
            for c in pdc:
                c.start()

        return carry

    lax.fori_loop(0, z_chunks + lag + defer, step, 0)

    def reduce_rest(g, carry):
        reduce_chip(g)
        return carry

    lax.fori_loop((z_chunks - 1 - reduce_lag) // per, groups, reduce_rest, 0)

    pivot_diag = pd_total(pd_own_c, pd_c, pdc_recv, x, n_cols)
    inverse[...] = 1.0 / jnp.sqrt(column_of(pivot_diag[0:1, :]))
    def each(count, wait):
        def one(q, carry):
            wait(q)
            return carry

        lax.fori_loop(0, count, one, 0)

    def finish(g, total_sq):
        total = mine[group_rows(g)]
        for c in range(1, n_cols):
            other = lax.rem(x + c, n_cols)
            arrived(col_in.at[other, group_rows(g)], col_recv.at[g, other])
            total = total + col_in[other, group_rows(g)]
        rows = group_rows(g)
        scale = inverse[rows, :]
        for h in range(rows_here // LANES):
            cut = slice(h * LANES, (h + 1) * LANES)
            scaled_t[rows, cut] = (prev_t[rows, cut] - total[:, cut]) * scale
        scaled = scaled_t[rows, :]
        return total_sq + jnp.sum(scaled * scaled, axis=0, keepdims=True)

    def write(first, count):
        done = slice(first, first + count)
        new_ref[:, done] = jnp.transpose(scaled_t[done, :]).astype(jnp.bfloat16)

    total_sq = jnp.zeros((1, rows_here), jnp.float32)
    early = (batch - 1) // LANES * LANES // g_rows
    total_sq = lax.fori_loop(0, early, finish, total_sq)
    if early:
        write(0, early * g_rows)
    total_sq = lax.fori_loop(early, last, finish, total_sq)

    for d in range(1, n_rows):
        other = lax.rem(z + d, n_rows)
        arrived(landed.at[other], ket_recv.at[other])
    for place in range(per_device):
        block = device * per_device + place
        source = jnp.int32(0)
        for band in range(n_rows):
            owner = band * column_size + column
            for slot in range(slot_count):
                fits = (slot < counts_ref[owner]) & (targets_ref[slot, owner] == block)
                source = jnp.where(fits, jnp.int32(band), source)
        next_ref[place * block_rows:(place + 1) * block_rows, :] = landed[source]

    for c in pdz + pds + pdc:
        c.wait_send()
    for d in range(1, n_rows):
        ket_copy(d).wait_send()

    @pl.when(z < n_rows - 1)
    def _():
        each(z_chunks, lambda q: z_copy(own, from_l, zr_send, l_recv, q, 1).wait_send())

    @pl.when(z > 0)
    def _():
        each(z_chunks, lambda q: z_copy(own, from_r, zl_send, r_recv, q, -1).wait_send())

    for d in range(1, n_sub):
        each(groups, lambda g: sub_copy(g, d).wait_send())
    for c in range(1, n_cols):
        each(last, lambda g: col_copy(g, c).wait_send())

    total_sq = finish(last, total_sq)
    write(early * g_rows, batch - early * g_rows)
    diag_out_ref[...] = diag_ref[...] - total_sq
    for c in range(1, n_cols):
        col_copy(last, c).wait_send()


def flush(new_ref, diag_ref, next_ref, new_hbm, diag_hbm, next_hbm, sem):
    copies = [
        pltpu.make_async_copy(new_ref, new_hbm, sem.at[0]),
        pltpu.make_async_copy(next_ref, next_hbm, sem.at[1]),
        pltpu.make_async_copy(diag_ref, diag_hbm, sem.at[2]),
    ]
    for c in copies:
        c.start()
    for c in copies:
        c.wait()


def body(mesh_sizes, vectors, previous, pivots, diagonal, ket_blocks, tags, targets, counts, norms):
    n_rows, n_cols, n_sub = mesh_sizes
    width, band_rows = vectors.shape
    rows_here, batch = previous.shape
    slot_count, block_rows, _ = ket_blocks.shape
    z_chunks, hop_lead, hop_bias = 16, (7, 5), 1
    z_rows, m_chunks = batch // z_chunks, z_chunks // PER
    f32, bf16, dma = jnp.float32, jnp.bfloat16, pltpu.SemaphoreType.DMA
    line = pltpu.VMEM((z_chunks, z_rows, width), bf16)
    small = pltpu.VMEM((1, batch), f32)
    scratch = [
        pltpu.VMEM((1, batch), jnp.int32), pltpu.VMEM((1, rows_here), f32),
        pltpu.VMEM(tags.shape, jnp.int32), pltpu.SMEM(targets.shape[::-1], jnp.int32),
        pltpu.SMEM(counts.shape, jnp.int32), pltpu.SMEM(norms.shape, f32),
        pltpu.VMEM(vectors.shape, bf16), pltpu.VMEM(previous.shape, bf16),
        pltpu.VMEM(ket_blocks.shape, bf16), pltpu.VMEM((batch, band_rows), bf16),
        line, line, line, line, line, line,
        pltpu.VMEM((batch, rows_here), f32),
        pltpu.VMEM((n_sub, n_cols * batch, rows_here), f32),
        pltpu.VMEM((n_sub, n_cols * batch, rows_here), f32),
        pltpu.VMEM((batch, rows_here), f32),
        pltpu.VMEM((n_cols, batch, rows_here), f32),
        pltpu.VMEM((n_cols, batch, rows_here), f32),
        pltpu.VMEM((batch, rows_here), f32), pltpu.VMEM((batch, LANES), f32),
        pltpu.VMEM((n_rows, block_rows, batch), bf16),
        pltpu.VMEM((n_rows, block_rows, batch), bf16),
        pltpu.VMEM((n_rows + 1, 1, batch), f32), pltpu.VMEM((n_sub, 1, batch), f32),
        pltpu.VMEM((n_cols, 1, batch), f32), small, small,
        dma((8,)), dma((max(width // PART, 1),)), dma((z_chunks,)), dma((z_chunks,)), dma((z_chunks,)), dma((z_chunks,)),
        dma((m_chunks, n_sub)), dma((m_chunks, n_sub)),
        dma((m_chunks, n_cols)), dma((m_chunks, n_cols)),
        dma((n_rows,)), dma((n_rows,)), dma((n_rows,)), dma((n_rows,)),
        dma((n_sub,)), dma((n_sub,)), dma((n_cols,)), dma((n_cols,)),
    ]
    hbm = pl.BlockSpec(memory_space=pl.ANY)
    vmem = pl.BlockSpec(memory_space=pltpu.VMEM)
    new_vectors, diag_out, next_columns = pl.pallas_call(
        functools.partial(kernel, (n_rows, n_cols, n_sub, hop_lead, hop_bias, PER)),
        out_shape=(
            pltpu.VMEM((rows_here, batch), bf16),
            pltpu.VMEM((1, rows_here), f32),
            pltpu.VMEM((rows_here, batch), bf16),
        ),
        in_specs=[hbm] * 9,
        out_specs=(vmem, vmem, vmem),
        scratch_shapes=scratch,
        compiler_params=pltpu.CompilerParams(
            collective_id=0, has_side_effects=True, vmem_limit_bytes=63 * 1024 * 1024),
    )(
        vectors, previous, pivots.reshape(1, batch), diagonal.reshape(1, rows_here),
        ket_blocks, tags, targets.T, counts, norms,
    )
    new_vectors, diag_out, next_columns = pl.pallas_call(
        flush,
        out_shape=(
            jax.ShapeDtypeStruct((rows_here, batch), bf16),
            jax.ShapeDtypeStruct((1, rows_here), f32),
            jax.ShapeDtypeStruct((rows_here, batch), bf16),
        ),
        in_specs=[vmem] * 3,
        out_specs=(hbm, hbm, hbm),
        scratch_shapes=[dma((3,))],
        compiler_params=pltpu.CompilerParams(vmem_limit_bytes=1024 * 1024),
    )(new_vectors, diag_out, next_columns)
    return new_vectors, diag_out.reshape(rows_here), next_columns


def solution(mesh):
    sizes = tuple(mesh.shape[name] for name in ("rows", "cols", "sub"))
    return jax.shard_map(
        functools.partial(body, sizes),
        mesh=mesh,
        in_specs=(
            P(("cols", "sub"), ("groups", "rows")),
            P(("groups", "rows", "cols", "sub"), None),
            P("groups"),
            P(("groups", "rows", "cols", "sub")),
            P(("groups", "rows", "cols", "sub"), None, None),
            P(("groups", "rows", "cols", "sub"), None),
            P("groups", None),
            P("groups"),
            P(),
        ),
        out_specs=(
            P(("groups", "rows", "cols", "sub"), None),
            P(("groups", "rows", "cols", "sub")),
            P(("groups", "rows", "cols", "sub"), None),
        ),
        check_vma=False,
    )
```
